16 devices in a mesh: dp: 2 (over y, z), cp: 8 (over x, core).
Axes of the slice: x: 4, y: 2, z: 1, core: 2. Of those that a mesh axis runs over, the one named last changes fastest.
The devices are a block of a 4x4x8 slice.
Arguments:
- hidden: bfloat16 [16, 1024, 896], P('dp', 'cp'), parts along dimension 0
- positions: int32 [16, 1024], P('dp', 'cp'), parts along dimension 0
- norm_gain: bfloat16 [896], replicated
- w_query: bfloat16 [896, 896], replicated
- w_key: bfloat16 [896, 128], replicated
- w_value: bfloat16 [896, 128], replicated
- w_out: bfloat16 [14, 64, 896], replicated
Outputs:
- output: bfloat16 [16, 1024, 896], P('dp', 'cp'), parts along dimension 0
There are 2 independent parts. The reference program is written for one: setup_inputs(seed, part) draws one part's arguments, and reference() takes and returns one part's arrays. A program takes and returns all parts, laid end to end along the dimension named above; an argument that names none is the same for every part.
All inputs are finite; a program needn't handle non-finite values.
Results may differ from the reference program's by a relative error of at most 0.00739962.
Values are sent between devices in bfloat16 or wider.
A program may use at most 768 MiB of HBM per device.

```python
import jax
import jax.numpy as jnp
from jax import lax

BATCH = 8
SEQ = 1024
QBLOCK = 128
D = 896
HEADS = 14
KV_HEADS = 2
HEAD = 64

GROUPS = HEADS // KV_HEADS
NBLOCKS = SEQ // QBLOCK


def draw_positions(pos_key):
    off_key, stride_key = jax.random.split(pos_key)
    offsets = jax.random.randint(off_key, (BATCH, 1), 0, SEQ)
    strides = jax.random.randint(stride_key, (BATCH, SEQ), 1, 3)
    return (offsets + jnp.cumsum(strides, axis=1) - 1).astype(jnp.int32)


def normal_weight(weight_key, shape, scale):
    return (scale * jax.random.normal(weight_key, shape, jnp.float32)).astype(jnp.bfloat16)


def setup_inputs(seed: int = 0, part: int = 0) -> dict:
    root = jax.random.key(seed)
    part_key = jax.random.fold_in(root, part)
    shared = jax.random.fold_in(root, 1000003)
    hid_key, pos_key = jax.random.split(part_key)
    gain_key, q_key, k_key, v_key, o_key = jax.random.split(shared, 5)
    hidden = (0.25 * jax.random.normal(hid_key, (BATCH, SEQ, D), jnp.float32)).astype(jnp.bfloat16)
    norm_gain = (1.0 + 0.3 * jax.random.normal(gain_key, (D,), jnp.float32)).astype(jnp.bfloat16)
    return {
        'hidden': hidden,
        'positions': draw_positions(pos_key),
        'norm_gain': norm_gain,
        'w_query': normal_weight(q_key, (D, HEADS * HEAD), 1.3 * D ** -0.5),
        'w_key': normal_weight(k_key, (D, KV_HEADS * HEAD), 1.3 * D ** -0.5),
        'w_value': normal_weight(v_key, (D, KV_HEADS * HEAD), D ** -0.5),
        'w_out': normal_weight(o_key, (HEADS, HEAD, D), 2.0 * (HEADS * HEAD) ** -0.5),
    }


def rms_norm(hidden, norm_gain):
    x_f32 = hidden.astype(jnp.float32)
    inv_rms = lax.rsqrt(jnp.mean(x_f32 * x_f32, axis=-1, keepdims=True) + 1e-5)
    return (x_f32 * inv_rms * norm_gain.astype(jnp.float32)).astype(jnp.bfloat16)


def rotary(proj_f32, positions):
    head_dim = proj_f32.shape[-1]
    half_dim = head_dim // 2
    inv_freq = 10000.0 ** (-2.0 * jnp.arange(half_dim, dtype=jnp.float32) / head_dim)
    angles = positions.astype(jnp.float32)[:, :, None] * inv_freq
    cos_part = jnp.cos(angles)[:, :, None, :]
    sin_part = jnp.sin(angles)[:, :, None, :]
    first_half = proj_f32[..., :half_dim]
    second_half = proj_f32[..., half_dim:]
    return jnp.concatenate([first_half * cos_part - second_half * sin_part, second_half * cos_part + first_half * sin_part], axis=-1).astype(jnp.bfloat16)


def reference(hidden, positions, norm_gain, w_query, w_key, w_value, w_out):
    normed = rms_norm(hidden, norm_gain).reshape(BATCH * SEQ, D)
    q_rot = rotary(jnp.dot(normed, w_query, preferred_element_type=jnp.float32).reshape(BATCH, SEQ, HEADS, HEAD), positions)
    k_rot = rotary(jnp.dot(normed, w_key, preferred_element_type=jnp.float32).reshape(BATCH, SEQ, KV_HEADS, HEAD), positions)
    v_all = jnp.dot(normed, w_value, preferred_element_type=jnp.float32).astype(jnp.bfloat16).reshape(BATCH, SEQ, KV_HEADS, HEAD)
    q_grp = q_rot.reshape(BATCH, SEQ, KV_HEADS, GROUPS, HEAD).astype(jnp.float32)
    k_f32 = k_rot.astype(jnp.float32)
    v_f32 = v_all.astype(jnp.float32)
    w_out_grp = w_out.reshape(KV_HEADS, GROUPS, HEAD, D).astype(jnp.float32)
    token_idx = jnp.arange(QBLOCK)

    def query_block(query_idx):
        q_blk = lax.dynamic_slice_in_dim(q_grp, query_idx * QBLOCK, QBLOCK, axis=1)

        def key_step(att_state, key_idx):
            def consume(state_in):
                run_max, run_sum, acc_out = state_in
                k_blk = lax.dynamic_slice_in_dim(k_f32, key_idx * QBLOCK, QBLOCK, axis=1)
                v_blk = lax.dynamic_slice_in_dim(v_f32, key_idx * QBLOCK, QBLOCK, axis=1)
                scores = jnp.einsum('bqkgd,bskd->bkgqs', q_blk, k_blk) * (HEAD ** -0.5)
                allowed = (query_idx * QBLOCK + token_idx)[:, None] >= (key_idx * QBLOCK + token_idx)[None, :]
                scores = jnp.where(allowed, scores, -jnp.inf)
                new_max = jnp.maximum(run_max, jnp.max(scores, axis=-1))
                prob_blk = jnp.exp(scores - new_max[..., None])
                rescale = jnp.exp(run_max - new_max)
                new_sum = run_sum * rescale + jnp.sum(prob_blk, axis=-1)
                new_acc = acc_out * rescale[..., None] + jnp.einsum('bkgqs,bskd->bkgqd', prob_blk, v_blk)
                return new_max, new_sum, new_acc
            return lax.cond(key_idx <= query_idx, consume, lambda state_kept: state_kept, att_state), None

        start_state = (
            jnp.full((BATCH, KV_HEADS, GROUPS, QBLOCK), -jnp.inf, jnp.float32),
            jnp.zeros((BATCH, KV_HEADS, GROUPS, QBLOCK), jnp.float32),
            jnp.zeros((BATCH, KV_HEADS, GROUPS, QBLOCK, HEAD), jnp.float32),
        )
        final_state, _ = lax.scan(key_step, start_state, jnp.arange(NBLOCKS))
        attn_out = (final_state[2] / final_state[1][..., None]).astype(jnp.bfloat16).astype(jnp.float32)
        x_blk = lax.dynamic_slice_in_dim(hidden, query_idx * QBLOCK, QBLOCK, axis=1).astype(jnp.float32)
        return (x_blk + jnp.einsum('bkgqd,kgde->bqe', attn_out, w_out_grp)).astype(jnp.bfloat16)

    out_blocks = lax.map(query_block, jnp.arange(NBLOCKS))
    return jnp.moveaxis(out_blocks, 0, 1).reshape(BATCH, SEQ, D)
```

```python
import functools

import jax
import jax.numpy as jnp
import numpy as np
from jax import lax
from jax.experimental import pallas as pl
from jax.experimental.pallas import tpu as pltpu
from jax.sharding import PartitionSpec as P

F32 = jnp.float32
BF16 = jnp.bfloat16
MESH = pl.DeviceIdType.MESH
S_PART, S_RIGHT, S_LEFT, S_RELAY, S_FWD = 0, 1, 2, 3, 4
AHEAD = 3


def tdot(lhs, rhs, dims):
    return lax.dot_general(lhs, rhs, (dims, ((), ())), preferred_element_type=F32)


def rope(proj, cos, sin):
    half = cos.shape[0]
    first, second = proj[:half], proj[half:]
    return jnp.concatenate([first * cos - second * sin, second * cos + first * sin], axis=0).astype(BF16)


def block_kernel(n_cp, x_hbm, pos_ref, gain_ref, freq_ref, wq_hbm, wk_hbm, wv_hbm, wo_hbm, y_hbm,
                 x_s, wq_s, wk_s, wv_s, wo_s, cos_s, sin_s, q_s, kv_s, score_s, bias_s, ot_s, y_s,
                 x_sem, w_sem, y_sem, send_sem, recv_sem):
    batch, tok, dim = x_hbm.shape
    head = 2 * freq_ref.shape[0]
    n_heads = wq_hbm.shape[1] // head
    n_kv = wk_hbm.shape[1] // head
    group = n_heads // n_kv
    n_pairs = n_heads // 2
    n_chips = n_cp // 2
    scale = float(head ** -0.5 * np.log2(np.e))

    me = lax.axis_index('cp')
    chip = me // 2
    core = me % 2
    partner = chip * 2 + 1 - core

    def x_copy(b):
        return pltpu.make_async_copy(x_hbm.at[b], x_s.at[b], x_sem.at[b])

    w_copies = [pltpu.make_async_copy(src, dst, w_sem.at[i]) for i, (src, dst) in enumerate(
        ((wk_hbm, wk_s), (wv_hbm, wv_s), (wq_hbm, wq_s), (wo_hbm, wo_s)))]
    x_copy(0).start()
    x_copy(1).start()
    w_copies[0].start()
    w_copies[1].start()
    w_copies[2].start()
    for b in range(2, batch):
        x_copy(b).start()
    w_copies[3].start()

    barrier = pltpu.get_barrier_semaphore()
    for d in range(1, n_cp):
        pl.semaphore_signal(barrier, inc=1, device_id={'cp': lax.rem(me + d, n_cp)}, device_id_type=MESH)

    for b in range(batch):
        angle = pos_ref[pl.ds(b, 1), :].astype(F32) * freq_ref[...]
        cos_s[:, b * tok:(b + 1) * tok] = jnp.cos(angle)
        sin_s[:, b * tok:(b + 1) * tok] = jnp.sin(angle)
    q_s[...] = jnp.zeros_like(q_s)
    key_i = lax.broadcasted_iota(jnp.int32, bias_s.shape, 0)
    tok_i = lax.broadcasted_iota(jnp.int32, bias_s.shape, 1)
    bias_s[...] = jnp.where(key_i <= tok_i + core * tok, 0.0, -jnp.inf).astype(F32)

    pl.semaphore_wait(barrier, n_cp - 1)

    def send(b, src, dst, kind):
        return pltpu.make_async_remote_copy(
            src_ref=kv_s.at[b, src], dst_ref=kv_s.at[b, src],
            send_sem=send_sem.at[kind, b], recv_sem=recv_sem.at[b, src],
            device_id={'cp': dst}, device_id_type=MESH)

    def wait_recv(b, src):
        send(b, src, partner, S_PART).wait_recv()

    def via_left(b):
        return (b + core) % 2 == 1

    def each_own(b, do):
        do(send(b, me, partner, S_PART))

        @pl.when(chip == 0)
        def _():
            do(send(b, me, 6 + core, S_LEFT))
            do(send(b, me, 2 + core, S_RIGHT))

        @pl.when(chip == 1)
        def _():
            @pl.when(via_left(b))
            def _():
                do(send(b, me, core, S_LEFT))
            do(send(b, me, 4 + core, S_RIGHT))

        @pl.when(chip == 2)
        def _():
            do(send(b, me, 6 + core, S_RIGHT))

    def relays(b, first, then):
        def forward(c):
            then(send(b, 2 * c + core, partner, S_FWD + c))

        @pl.when(chip == 0)
        def _():
            @pl.when(via_left(b))
            def _():
                first(2 + core)
                then(send(b, 2 + core, 6 + core, S_RELAY))

        @pl.when(chip == 1)
        def _():
            first(core)
            forward(0)

        @pl.when(chip == 2)
        def _():
            first(2 + core)

            @pl.when(jnp.logical_not(via_left(b)))
            def _():
                then(send(b, 2 + core, 6 + core, S_RELAY))
            forward(1)
            first(core)
            forward(0)

        @pl.when(chip == 3)
        def _():
            first(core)
            then(send(b, core, 4 + core, S_RELAY))
            forward(0)
            first(4 + core)
            forward(2)
            first(2 + core)
            forward(1)

    w_copies[0].wait()
    w_copies[1].wait()

    def project(p, first_pair):
        for i in range(2):
            x_copy(2 * p + i).wait()
        x_pair = x_s[pl.ds(2 * p, 2)].reshape(2 * tok, dim).astype(F32)
        inv_rms = lax.rsqrt(jnp.mean(x_pair * x_pair, axis=-1, keepdims=True) + 1e-5)
        normed = (x_pair * inv_rms * gain_ref[...].astype(F32)).astype(BF16)
        lanes = pl.ds(pl.multiple_of(p * 2 * tok, 2 * tok), 2 * tok)
        cos, sin = cos_s[:, lanes], sin_s[:, lanes]
        k_t = tdot(wk_s[...], normed, ((0,), (1,)))
        v_t = tdot(wv_s[...], normed, ((0,), (1,))).astype(BF16)
        k_rot = jnp.concatenate([rope(k_t[g * head:(g + 1) * head], cos, sin) for g in range(n_kv)], axis=0)
        for i in range(2):
            kv_s[2 * p + i, me, 0] = k_rot[:, i * tok:(i + 1) * tok].T
            kv_s[2 * p + i, me, 1] = v_t[:, i * tok:(i + 1) * tok]
        for i in range(2):
            @pl.when(2 * p + i < AHEAD)
            def _():
                each_own(2 * p + i, lambda copy: copy.start())
        if first_pair:
            w_copies[2].wait()
        q_t = tdot(wq_s[...], normed, ((0,), (1,)))
        for n in range(n_heads):
            q_rot = rope(q_t[n * head:(n + 1) * head], cos, sin)
            row = (n // group) * head
            col = (n % 2) * tok
            for i in range(2):
                q_s[2 * p + i, n // 2, row:row + head, col:col + tok] = q_rot[:, i * tok:(i + 1) * tok]

    project(0, True)

    @pl.loop(1, batch // 2)
    def _(p):
        project(p, False)

    w_copies[3].wait()

    def attend(b, chunks):
        keys = 2 * tok * chunks
        for t in range(n_pairs):
            q_pair = q_s[b, t]
            slot = t % 2
            for c in range(chunks):
                k_blk = jnp.concatenate([kv_s[b, 2 * c, 0], kv_s[b, 2 * c + 1, 0]], axis=0)
                s_blk = tdot(k_blk, q_pair, ((1,), (0,)))
                if c == chunks - 1:
                    bias = bias_s[...]
                    s_blk = s_blk + jnp.concatenate([bias, bias], axis=1)
                score_s[slot, 2 * tok * c:2 * tok * (c + 1)] = s_blk
                part = jnp.max(s_blk, axis=0, keepdims=True)
                top = part if c == 0 else jnp.maximum(top, part)
            prob = jnp.exp2((score_s[slot, :keys] - top) * scale)
            total = jnp.sum(prob, axis=0, keepdims=True)
            lo, hi = (2 * t) // group, (2 * t + 1) // group
            v_rows = slice(lo * head, (hi + 1) * head)
            v_blk = jnp.concatenate([kv_s[b, s, 1][v_rows] for s in range(2 * chunks)], axis=1)
            out = tdot(v_blk, prob.astype(BF16), ((1,), (0,)))
            inv = 1.0 / total
            for i in range(2):
                n = 2 * t + i
                row = (n // group - lo) * head
                cols = slice(i * tok, (i + 1) * tok)
                ot_s[n * head:(n + 1) * head] = (out[row:row + head, cols] * inv[:, cols]).astype(BF16)

    def y_copy(b):
        return pltpu.make_async_copy(y_s.at[b], y_hbm.at[b], y_sem.at[b])

    @pl.loop(0, batch)
    def _(b):
        relays(b, lambda src: wait_recv(b, src), lambda copy: copy.start())

        @pl.when(b + AHEAD < batch)
        def _():
            each_own(b + AHEAD, lambda copy: copy.start())
        wait_recv(b, partner)
        for j in range(n_chips):
            @pl.when(chip == j)
            def _():
                for c in range(j):
                    wait_recv(b, 2 * c + 1 - core)
                attend(b, j + 1)
        proj = tdot(ot_s[...], wo_s[...], ((0,), (0,)))
        y_s[b] = (x_s[b].astype(F32) + proj).astype(BF16)
        y_copy(b).start()

    @pl.loop(0, batch)
    def _(b):
        y_copy(b).wait()
        each_own(b, lambda copy: copy.wait_send())
        relays(b, lambda src: None, lambda copy: copy.wait_send())


def solution(mesh):
    n_cp = mesh.shape['cp']

    def local_block(hidden, positions, norm_gain, w_query, w_key, w_value, w_out):
        batch, tok, dim = hidden.shape
        n_heads, head, _ = w_out.shape
        kv_dim = w_key.shape[1]
        freq = np.float32(10000.0) ** (np.float32(-2.0) * np.arange(head // 2, dtype=np.float32) / np.float32(head))
        freq = jnp.asarray(np.broadcast_to(freq.astype(np.float32)[:, None], (head // 2, tok)))
        hbm = pl.BlockSpec(memory_space=pl.ANY)
        vmem = pl.BlockSpec(memory_space=pltpu.VMEM)
        flops = 2 * batch * tok * dim * (2 * dim + 2 * kv_dim) + 4 * batch * tok * n_cp * tok * n_heads * head
        return pl.pallas_call(
            functools.partial(block_kernel, n_cp),
            name='attention_block',
            out_shape=jax.ShapeDtypeStruct(hidden.shape, hidden.dtype),
            in_specs=[hbm, vmem, vmem, vmem, hbm, hbm, hbm, hbm],
            out_specs=hbm,
            scratch_shapes=[
                pltpu.VMEM(hidden.shape, BF16),
                pltpu.VMEM(w_query.shape, BF16),
                pltpu.VMEM(w_key.shape, BF16),
                pltpu.VMEM(w_value.shape, BF16),
                pltpu.VMEM((n_heads * head, dim), BF16),
                pltpu.VMEM((head // 2, batch * tok), F32),
                pltpu.VMEM((head // 2, batch * tok), F32),
                pltpu.VMEM((batch, n_heads // 2, kv_dim, 2 * tok), BF16),
                pltpu.VMEM((batch, n_cp, 2, tok, kv_dim), BF16),
                pltpu.VMEM((2, n_cp * tok, 2 * tok), F32),
                pltpu.VMEM((2 * tok, tok), F32),
                pltpu.VMEM((n_heads * head, tok), BF16),
                pltpu.VMEM(hidden.shape, BF16),
                pltpu.SemaphoreType.DMA((batch,)),
                pltpu.SemaphoreType.DMA((4,)),
                pltpu.SemaphoreType.DMA((batch,)),
                pltpu.SemaphoreType.DMA((S_FWD + n_cp // 2 - 1, batch)),
                pltpu.SemaphoreType.DMA((batch, n_cp)),
            ],
            compiler_params=pltpu.CompilerParams(
                collective_id=0, has_side_effects=True, vmem_limit_bytes=56 * 1024 * 1024),
            cost_estimate=pl.CostEstimate(flops=flops, bytes_accessed=8_000_000, transcendentals=0),
        )(hidden, positions, norm_gain.reshape(1, dim), freq, w_query, w_key, w_value, w_out.reshape(n_heads * head, dim))

    act_spec = P('dp', 'cp', None)
    return jax.shard_map(local_block, mesh=mesh, in_specs=(act_spec, P('dp', 'cp'), P(), P(), P(), P(), P()), out_specs=act_spec, check_vma=False)
```

```python
import functools

import jax
import jax.numpy as jnp
import numpy as np
from jax import lax
from jax.experimental import pallas as pl
from jax.experimental.pallas import tpu as pltpu
from jax.sharding import PartitionSpec as P

F32 = jnp.float32
BF16 = jnp.bfloat16
MESH = pl.DeviceIdType.MESH
S_PART, S_RIGHT, S_LEFT, S_FAR, S_RELAY, S_FWD = 0, 1, 2, 3, 4, 5
AHEAD = 3
PACED = (2, 2, 4, 2)
SPLIT = 4


def tdot(lhs, rhs, dims):
    return lax.dot_general(lhs, rhs, (dims, ((), ())), preferred_element_type=F32)


def rope(proj, cos, sin):
    half = cos.shape[0]
    first, second = proj[:half], proj[half:]
    return jnp.concatenate([first * cos - second * sin, second * cos + first * sin], axis=0).astype(BF16)


def block_kernel(n_cp, head, x_hbm, pos_hbm, gain_hbm, wq_hbm, wk_hbm, wv_hbm, wo_hbm, y_ref,
                 pos_ref, gain_ref, freq_s, x_s, wq_s, wk_s, wv_s, wo_s, q_s, kv_s, score_s, bias_s, o_s,
                 x_sem, w_sem, send_sem, recv_sem):
    batch, tok, dim = x_hbm.shape
    kv_dim = wk_hbm.shape[1]
    n_kv = kv_dim // head
    n_heads = wq_hbm.shape[1] // head
    group = n_heads // n_kv
    n_pairs = n_heads // 2
    n_chips = n_cp // 2
    scale = float(head ** -0.5 * np.log2(np.e))

    me = lax.axis_index('cp')
    chip = me // 2
    core = me % 2
    partner = chip * 2 + 1 - core

    def x_copy(b):
        return pltpu.make_async_copy(x_hbm.at[b], x_s.at[b], x_sem.at[b])

    w_copies = [pltpu.make_async_copy(src, dst, w_sem.at[i]) for i, (src, dst) in enumerate(
        ((wk_hbm, wk_s), (wv_hbm, wv_s), (wq_hbm, wq_s), (wo_hbm, wo_s), (pos_hbm, pos_ref), (gain_hbm, gain_ref)))]
    w_copies[4].start()
    x_copy(0).start()
    x_copy(1).start()
    w_copies[5].start()
    w_copies[0].start()
    w_copies[1].start()
    w_copies[2].start()
    for b in range(2, batch):
        x_copy(b).start()
    w_copies[3].start()

    barrier = pltpu.get_barrier_semaphore()
    for d in range(1, n_cp):
        pl.semaphore_signal(barrier, inc=1, device_id={'cp': lax.rem(me + d, n_cp)}, device_id_type=MESH)

    key_i = lax.broadcasted_iota(jnp.int32, bias_s.shape, 0)
    tok_i = lax.broadcasted_iota(jnp.int32, bias_s.shape, 1)
    bias_s[...] = jnp.where(key_i <= tok_i + core * tok, 0.0, -jnp.inf).astype(F32)

    def send(b, src, dst, kind):
        return pltpu.make_async_remote_copy(
            src_ref=kv_s.at[b, src], dst_ref=kv_s.at[b, src],
            send_sem=send_sem.at[kind, b], recv_sem=recv_sem.at[b, src],
            device_id={'cp': dst}, device_id_type=MESH)

    def wait_recv(b, src):
        send(b, src, partner, S_PART).wait_recv()

    def on_chip(do):
        for j in range(n_chips):
            @pl.when(chip == j)
            def _():
                do(j)

    def direct_0_to_2(b):
        return (b < 2) | (b >= 6)

    def direct_1_to_3(b):
        return b < 4

    def own(j, b, do):
        if j == 0:
            do(send(b, me, 6 + core, S_LEFT))
            do(send(b, me, 2 + core, S_RIGHT))

            @pl.when(direct_0_to_2(b))
            def _():
                do(send(b, me, 4 + core, S_FAR))
        if j == 1:
            @pl.when(direct_1_to_3(b))
            def _():
                do(send(b, me, 6 + core, S_FAR))
            do(send(b, me, 4 + core, S_RIGHT))
        if j == 2:
            do(send(b, me, 6 + core, S_RIGHT))

    def stages(j, first, then):
        def forward(b, c):
            then(send(b, 2 * c + core, partner, S_FWD + c))

        def near(b):
            first(b, 2 * (j - 1) + core)
            forward(b, j - 1)

        def chip_2_right(b):
            first(b, 2 + core)

            @pl.when(jnp.logical_not(direct_1_to_3(b)))
            def _():
                then(send(b, 2 + core, 6 + core, S_RELAY))
            forward(b, 1)

        def chip_2_left(b):
            first(b, core)
            forward(b, 0)

        def chip_3(b):
            first(b, core)

            @pl.when(jnp.logical_not(direct_0_to_2(b)))
            def _():
                then(send(b, core, 4 + core, S_RELAY))
            forward(b, 0)
            near(b)
            first(b, 2 + core)
            forward(b, 1)

        return ((), ((1, near),), ((AHEAD, chip_2_right), (1, chip_2_left)), ((1, chip_3),))[j]

    w_copies[4].wait()
    w_copies[5].wait()
    row_i = lax.broadcasted_iota(jnp.int32, (head // 2, 2 * tok), 0)
    freq = jnp.ones((head // 2, 2 * tok), F32)
    for j in range(1, head // 2):
        freq = jnp.where(row_i == j, F32(10000.0 ** (-2.0 * j / head)), freq)
    freq_s[...] = freq
    w_copies[0].wait()
    w_copies[1].wait()

    def project(p, first_pair):
        for i in range(2):
            x_copy(2 * p + i).wait()
        x_pair = x_s[pl.ds(2 * p, 2)].reshape(2 * tok, dim).astype(F32)
        inv_rms = lax.rsqrt(jnp.mean(x_pair * x_pair, axis=-1, keepdims=True) + 1e-5)
        normed = (x_pair * inv_rms * gain_ref[...].astype(F32).reshape(1, dim)).astype(BF16)
        pos = jnp.concatenate([pos_ref[pl.ds(2 * p + i, 1), :] for i in range(2)], axis=1)
        angle = pos.astype(F32) * freq_s[...]
        cos, sin = jnp.cos(angle), jnp.sin(angle)
        k_t = tdot(wk_s[...], normed, ((0,), (1,)))
        v_t = tdot(wv_s[...], normed, ((0,), (1,))).astype(BF16)
        k_rot = jnp.concatenate([rope(k_t[g * head:(g + 1) * head], cos, sin) for g in range(n_kv)], axis=0)
        for i in range(2):
            kv_s[2 * p + i, me, 0] = k_rot[:, i * tok:(i + 1) * tok].T
            kv_s[2 * p + i, me, 1] = v_t[:, i * tok:(i + 1) * tok]
        if first_pair:
            pl.semaphore_wait(barrier, n_cp - 1)

        def start_own(j):
            for i in range(2):
                @pl.when(2 * p + i < PACED[j])
                def _():
                    own(j, 2 * p + i, lambda copy: copy.start())
                send(2 * p + i, me, partner, S_PART).start()
        on_chip(start_own)
        if first_pair:
            w_copies[2].wait()
        q_t = tdot(wq_s[...], normed, ((0,), (1,)))
        zeros = jnp.zeros((head, tok), BF16)
        for n in range(n_heads):
            q_rot = rope(q_t[n * head:(n + 1) * head], cos, sin).astype(F32) * scale
            high = q_rot.astype(BF16)
            low = (q_rot - high.astype(F32)).astype(BF16)
            col = (n % 2) * tok
            for i in range(2):
                for part, q_part in enumerate((high, low)):
                    for g in range(n_kv):
                        q_s[2 * p + i, n // 2, part, g * head:(g + 1) * head, col:col + tok] = (
                            q_part[:, i * tok:(i + 1) * tok] if g == n // group else zeros)

    project(0, True)

    @pl.loop(1, batch // 2)
    def _(p):
        project(p, False)

    w_copies[3].wait()

    def scores(b, t, c, chunks):
        k_blk = jnp.concatenate([kv_s[b, 2 * c, 0], kv_s[b, 2 * c + 1, 0]], axis=0)
        s_blk = tdot(jnp.concatenate([k_blk, k_blk], axis=1), q_s[b, t].reshape(2 * kv_dim, 2 * tok), ((1,), (0,)))
        if c == chunks - 1:
            bias = bias_s[...]
            s_blk = s_blk + jnp.concatenate([bias, bias], axis=1)
        score_s[t % 2, 2 * tok * c:2 * tok * (c + 1)] = s_blk
        return jnp.max(s_blk, axis=0, keepdims=True)

    def attend(b, chunks, between):
        top = functools.reduce(jnp.maximum, [scores(b, 0, c, chunks) for c in range(chunks)])
        for t in range(n_pairs):
            if t == SPLIT:
                between()
            probs, total, next_top = [], None, None
            for c in range(chunks):
                if t + 1 < n_pairs:
                    part = scores(b, t + 1, c, chunks)
                    next_top = part if c == 0 else jnp.maximum(next_top, part)
                prob = jnp.exp2(score_s[t % 2, 2 * tok * c:2 * tok * (c + 1)] - top)
                part = jnp.sum(prob, axis=0, keepdims=True)
                total = part if c == 0 else total + part
                probs.append(prob)
            lo, hi = (2 * t) // group, (2 * t + 1) // group
            v_rows = slice(lo * head, (hi + 1) * head)
            v_blk = jnp.concatenate([kv_s[b, s, 1][v_rows] for s in range(2 * chunks)], axis=1)
            out = tdot(v_blk, jnp.concatenate(probs, axis=0), ((1,), (0,)))
            inv = 1.0 / total
            halves = []
            for i in range(2):
                row = ((2 * t + i) // group - lo) * head
                cols = slice(i * tok, (i + 1) * tok)
                halves.append(out[row:row + head, cols] * inv[:, cols])
            o_s[:, 2 * t * head:2 * (t + 1) * head] = jnp.concatenate(halves, axis=0).T.astype(BF16)
            top = next_top

    def pass_on(j):
        return stages(j, wait_recv, lambda copy: copy.start())

    def prologue(j):
        for ahead, stage in pass_on(j):
            for b in range(ahead):
                stage(jnp.int32(b))

    on_chip(prologue)

    @pl.loop(0, batch)
    def _(b):
        def one_chip(j):
            @pl.when(b + PACED[j] < batch)
            def _():
                own(j, b + PACED[j], lambda copy: copy.start())
            wait_recv(b, partner)
            for c in range(j):
                wait_recv(b, 2 * c + 1 - core)

            def between():
                for ahead, stage in pass_on(j):
                    @pl.when(b + ahead < batch)
                    def _():
                        stage(b + ahead)
            attend(b, j + 1, between)

        on_chip(one_chip)
        proj = tdot(o_s[...], wo_s[...], ((1,), (0,)))
        y_ref[b] = (x_s[b].astype(F32) + proj).astype(BF16)

    @pl.loop(0, batch)
    def _(b):
        def one_chip(j):
            send(b, me, partner, S_PART).wait_send()
            own(j, b, lambda copy: copy.wait_send())
            for _, stage in stages(j, lambda b, src: None, lambda copy: copy.wait_send()):
                stage(b)
        on_chip(one_chip)


def solution(mesh):
    n_cp = mesh.shape['cp']

    def local_block(hidden, positions, norm_gain, w_query, w_key, w_value, w_out):
        batch, tok, dim = hidden.shape
        n_heads, head, _ = w_out.shape
        kv_dim = w_key.shape[1]
        hbm = pl.BlockSpec(memory_space=pltpu.HBM)
        vmem = pl.BlockSpec(memory_space=pltpu.VMEM)
        flops = 2 * batch * tok * dim * (2 * dim + 2 * kv_dim) + 4 * batch * tok * n_cp * tok * n_heads * head
        return pl.pallas_call(
            functools.partial(block_kernel, n_cp, head),
            name='attention_block',
            out_shape=pltpu.VMEM(hidden.shape, hidden.dtype),
            in_specs=[hbm] * 7,
            out_specs=vmem,
            scratch_shapes=[
                pltpu.VMEM(positions.shape, jnp.int32),
                pltpu.VMEM(norm_gain.shape, BF16),
                pltpu.VMEM((head // 2, 2 * tok), F32),
                pltpu.VMEM(hidden.shape, BF16),
                pltpu.VMEM(w_query.shape, BF16),
                pltpu.VMEM(w_key.shape, BF16),
                pltpu.VMEM(w_value.shape, BF16),
                pltpu.VMEM((n_heads * head, dim), BF16),
                pltpu.VMEM((batch, n_heads // 2, 2, kv_dim, 2 * tok), BF16),
                pltpu.VMEM((batch, n_cp, 2, tok, kv_dim), BF16),
                pltpu.VMEM((2, n_cp * tok, 2 * tok), F32),
                pltpu.VMEM((2 * tok, tok), F32),
                pltpu.VMEM((tok, n_heads * head), BF16),
                pltpu.SemaphoreType.DMA((batch,)),
                pltpu.SemaphoreType.DMA((6,)),
                pltpu.SemaphoreType.DMA((S_FWD + n_cp // 2 - 1, batch)),
                pltpu.SemaphoreType.DMA((batch, n_cp)),
            ],
            compiler_params=pltpu.CompilerParams(
                collective_id=0, has_side_effects=True, vmem_limit_bytes=32 * 1024 * 1024),
            cost_estimate=pl.CostEstimate(flops=flops, bytes_accessed=8_000_000, transcendentals=0),
        )(*[pltpu.with_memory_space_constraint(arg, pltpu.HBM) for arg in (
            hidden, positions, norm_gain, w_query, w_key, w_value, w_out.reshape(n_heads * head, dim))])

    act_spec = P('dp', 'cp', None)
    return jax.shard_map(local_block, mesh=mesh, in_specs=(act_spec, P('dp', 'cp'), P(), P(), P(), P(), P()), out_specs=act_spec, check_vma=False)
```

```python
import functools

import jax
import jax.numpy as jnp
import numpy as np
from jax import lax
from jax.experimental import pallas as pl
from jax.experimental.pallas import tpu as pltpu
from jax.sharding import PartitionSpec as P

F32 = jnp.float32
BF16 = jnp.bfloat16
MESH = pl.DeviceIdType.MESH
S_PART, S_RIGHT, S_LEFT, S_FAR, S_RELAY, S_FWD = 0, 1, 2, 3, 4, 5
AHEAD_2, AHEAD_3 = 3, 2
PACED = (3, 2, 3, 2)
FAR_0_TO_2 = (3, 4, 6, 7)
FAR_1_TO_3 = (5, 6, 7)
HALF_FAR_1_TO_3 = (0, 3, 4)


def one_of(b, numbers):
    return functools.reduce(jnp.logical_or, [b == number for number in numbers], b < 0)


SPLIT = 2


def tdot(lhs, rhs, dims):
    return lax.dot_general(lhs, rhs, (dims, ((), ())), preferred_element_type=F32)


def rope(proj, cos, sin):
    half = cos.shape[0]
    first, second = proj[:half], proj[half:]
    return jnp.concatenate([first * cos - second * sin, second * cos + first * sin], axis=0).astype(BF16)


def block_kernel(n_cp, head, x_hbm, pos_hbm, gain_hbm, wq_hbm, wk_hbm, wv_hbm, wo_hbm, y_ref,
                 pos_ref, gain_ref, freq_s, cos_s, sin_s, normed_s, x_s, wq_s, wk_s, wv_s, wo_s, q_s, kv_s, score_s, bias_s, o_s,
                 x_sem, w_sem, send_sem, recv_sem):
    batch, tok, dim = x_hbm.shape
    kv_dim = wk_hbm.shape[1]
    n_kv = kv_dim // head
    n_heads = wq_hbm.shape[1] // head
    group = n_heads // n_kv
    n_pairs = n_heads // 2
    n_chips = n_cp // 2
    scale = float(head ** -0.5 * np.log2(np.e))

    me = lax.axis_index('cp')
    chip = me // 2
    core = me % 2
    partner = chip * 2 + 1 - core

    def x_copy(b):
        return pltpu.make_async_copy(x_hbm.at[b], x_s.at[b], x_sem.at[b])

    w_copies = [pltpu.make_async_copy(src, dst, w_sem.at[i]) for i, (src, dst) in enumerate(
        ((wk_hbm, wk_s), (wv_hbm, wv_s), (wq_hbm, wq_s), (wo_hbm, wo_s), (pos_hbm, pos_ref), (gain_hbm, gain_ref)))]
    w_copies[4].start()
    x_copy(0).start()
    x_copy(1).start()
    w_copies[5].start()
    w_copies[0].start()
    w_copies[1].start()
    w_copies[2].start()
    for b in range(2, batch):
        x_copy(b).start()
    w_copies[3].start()

    barrier = pltpu.get_barrier_semaphore()
    for d in range(1, n_cp):
        pl.semaphore_signal(barrier, inc=1, device_id={'cp': lax.rem(me + d, n_cp)}, device_id_type=MESH)

    key_i = lax.broadcasted_iota(jnp.int32, bias_s.shape, 0)
    tok_i = lax.broadcasted_iota(jnp.int32, bias_s.shape, 1)
    bias_s[...] = jnp.where(key_i <= tok_i + core * tok, 0.0, -jnp.inf).astype(F32)

    def send(b, src, dst, kind):
        return pltpu.make_async_remote_copy(
            src_ref=kv_s.at[b, src], dst_ref=kv_s.at[b, src],
            send_sem=send_sem.at[kind, b], recv_sem=recv_sem.at[b, src],
            device_id={'cp': dst}, device_id_type=MESH)

    def wait_recv(b, src):
        send(b, src, partner, S_PART).wait_recv()

    def on_chip(do):
        for j in range(n_chips):
            @pl.when(chip == j)
            def _():
                do(j)

    def direct_0_to_2(b):
        return one_of(b, FAR_0_TO_2)

    def direct_1_to_3(b):
        return one_of(b, FAR_1_TO_3) | ((core == 0) & one_of(b, HALF_FAR_1_TO_3))

    def own(j, b, do):
        if j == 0:
            do(send(b, me, 6 + core, S_LEFT))
            do(send(b, me, 2 + core, S_RIGHT))

            @pl.when(direct_0_to_2(b))
            def _():
                do(send(b, me, 4 + core, S_FAR))
        if j == 1:
            @pl.when(direct_1_to_3(b))
            def _():
                do(send(b, me, 6 + core, S_FAR))
            do(send(b, me, 4 + core, S_RIGHT))
        if j == 2:
            do(send(b, me, 6 + core, S_RIGHT))

    def stages(j, first, then):
        def forward(b, c):
            then(send(b, 2 * c + core, partner, S_FWD + c))

        def near(b):
            first(b, 2 * (j - 1) + core)
            forward(b, j - 1)

        def chip_2_right(b):
            first(b, 2 + core)

            @pl.when(jnp.logical_not(direct_1_to_3(b)))
            def _():
                then(send(b, 2 + core, 6 + core, S_RELAY))
            forward(b, 1)

        def chip_2_left(b):
            first(b, core)
            forward(b, 0)

        def chip_3_left(b):
            first(b, core)

            @pl.when(jnp.logical_not(direct_0_to_2(b)))
            def _():
                then(send(b, core, 4 + core, S_RELAY))
            forward(b, 0)

        def chip_3_right(b):
            near(b)
            first(b, 2 + core)
            forward(b, 1)

        return ((), ((1, near),), ((AHEAD_2, chip_2_right), (1, chip_2_left)), ((AHEAD_3, chip_3_left), (1, chip_3_right)))[j]

    w_copies[4].wait()
    w_copies[5].wait()
    row_i = lax.broadcasted_iota(jnp.int32, (head // 2, 2 * tok), 0)
    freq = jnp.ones((head // 2, 2 * tok), F32)
    for j in range(1, head // 2):
        freq = jnp.where(row_i == j, F32(10000.0 ** (-2.0 * j / head)), freq)
    freq_s[...] = freq
    w_copies[0].wait()
    w_copies[1].wait()

    def project_kv(p):
        for i in range(2):
            x_copy(2 * p + i).wait()
        x_pair = x_s[pl.ds(2 * p, 2)].reshape(2 * tok, dim).astype(F32)
        inv_rms = lax.rsqrt(jnp.mean(x_pair * x_pair, axis=-1, keepdims=True) + 1e-5)
        normed = (x_pair * inv_rms * gain_ref[...].astype(F32).reshape(1, dim)).astype(BF16)
        pos = jnp.concatenate([pos_ref[pl.ds(2 * p + i, 1), :] for i in range(2)], axis=1)
        angle = pos.astype(F32) * freq_s[...]
        cos, sin = jnp.cos(angle), jnp.sin(angle)
        k_t = tdot(wk_s[...], normed, ((0,), (1,)))
        v_t = tdot(wv_s[...], normed, ((0,), (1,))).astype(BF16)
        k_rot = jnp.concatenate([rope(k_t[g * head:(g + 1) * head], cos, sin) for g in range(n_kv)], axis=0)
        for i in range(2):
            kv_s[2 * p + i, me, 0] = k_rot[:, i * tok:(i + 1) * tok].T
            kv_s[2 * p + i, me, 1] = v_t[:, i * tok:(i + 1) * tok]
        normed_s[p % 2] = normed
        cos_s[p % 2] = cos
        sin_s[p % 2] = sin

    def start_own(p):
        def start(j):
            for i in range(2):
                @pl.when(2 * p + i < PACED[j])
                def _():
                    own(j, 2 * p + i, lambda copy: copy.start())
                send(2 * p + i, me, partner, S_PART).start()
        on_chip(start)

    def project_q(p):
        cos, sin = cos_s[p % 2], sin_s[p % 2]
        q_t = tdot(wq_s[...], normed_s[p % 2], ((0,), (1,)))
        zeros = jnp.zeros((head, tok), BF16)
        for n in range(n_heads):
            q_rot = rope(q_t[n * head:(n + 1) * head], cos, sin)
            col = (n % 2) * tok
            for i in range(2):
                for g in range(n_kv):
                    q_s[2 * p + i, n // 2, g * head:(g + 1) * head, col:col + tok] = (
                        q_rot[:, i * tok:(i + 1) * tok] if g == n // group else zeros)

    project_kv(0)
    pl.semaphore_wait(barrier, n_cp - 1)
    start_own(0)
    w_copies[2].wait()

    @pl.loop(1, batch // 2)
    def _(p):
        project_kv(p)
        project_q(p - 1)
        start_own(p)

    project_q(batch // 2 - 1)
    w_copies[3].wait()

    units = [(t, min(2, n_pairs - t)) for t in range(0, n_pairs, 2)]

    def scores(b, u, c, chunks):
        first_t, width = units[u]
        k_blk = jnp.concatenate([kv_s[b, 2 * c, 0], kv_s[b, 2 * c + 1, 0]], axis=0)
        q_unit = jnp.concatenate([q_s[b, first_t + i] for i in range(width)], axis=1)
        s_blk = tdot(k_blk, q_unit, ((1,), (0,)))
        if c == chunks - 1:
            s_blk = s_blk + jnp.concatenate([bias_s[...]] * (2 * width), axis=1)
        score_s[u % 2, 2 * tok * c:2 * tok * (c + 1), :2 * tok * width] = s_blk
        return jnp.max(s_blk, axis=0, keepdims=True)

    def attend(b, chunks, between):
        top = functools.reduce(jnp.maximum, [scores(b, 0, c, chunks) for c in range(chunks)])
        for u, (first_t, width) in enumerate(units):
            if u == SPLIT:
                between()
            probs, total, next_top = [], None, None
            for c in range(chunks):
                if u + 1 < len(units):
                    part = scores(b, u + 1, c, chunks)
                    next_top = part if c == 0 else jnp.maximum(next_top, part)
                prob = jnp.exp2((score_s[u % 2, 2 * tok * c:2 * tok * (c + 1), :2 * tok * width] - top) * scale)
                part = jnp.sum(prob, axis=0, keepdims=True)
                total = part if c == 0 else total + part
                probs.append(prob)
            inv = 1.0 / total
            for w in range(width):
                t = first_t + w
                lo, hi = (2 * t) // group, (2 * t + 1) // group
                v_rows = slice(lo * head, (hi + 1) * head)
                v_blk = jnp.concatenate([kv_s[b, s, 1][v_rows] for s in range(2 * chunks)], axis=1)
                pair = slice(2 * tok * w, 2 * tok * (w + 1))
                out = tdot(v_blk, jnp.concatenate([prob[:, pair] for prob in probs], axis=0), ((1,), (0,)))
                out_inv = inv[:, pair]
                halves = []
                for i in range(2):
                    row = ((2 * t + i) // group - lo) * head
                    cols = slice(i * tok, (i + 1) * tok)
                    halves.append(out[row:row + head, cols] * out_inv[:, cols])
                o_s[:, 2 * t * head:2 * (t + 1) * head] = jnp.concatenate(halves, axis=0).T.astype(BF16)
            top = next_top

    def pass_on(j):
        return stages(j, wait_recv, lambda copy: copy.start())

    def prologue(j):
        for ahead, stage in pass_on(j):
            for b in range(ahead):
                stage(jnp.int32(b))

    on_chip(prologue)

    @pl.loop(0, batch)
    def _(b):
        def one_chip(j):
            @pl.when(b + PACED[j] < batch)
            def _():
                own(j, b + PACED[j], lambda copy: copy.start())
            wait_recv(b, partner)
            for c in range(j):
                wait_recv(b, 2 * c + 1 - core)

            def between():
                for ahead, stage in pass_on(j):
                    @pl.when(b + ahead < batch)
                    def _():
                        stage(b + ahead)
            attend(b, j + 1, between)

        on_chip(one_chip)
        proj = tdot(o_s[...], wo_s[...], ((1,), (0,)))
        y_ref[b] = (x_s[b].astype(F32) + proj).astype(BF16)

    @pl.loop(0, batch)
    def _(b):
        def one_chip(j):
            send(b, me, partner, S_PART).wait_send()
            own(j, b, lambda copy: copy.wait_send())
            for _, stage in stages(j, lambda b, src: None, lambda copy: copy.wait_send()):
                stage(b)
        on_chip(one_chip)


def solution(mesh):
    n_cp = mesh.shape['cp']

    def local_block(hidden, positions, norm_gain, w_query, w_key, w_value, w_out):
        batch, tok, dim = hidden.shape
        n_heads, head, _ = w_out.shape
        kv_dim = w_key.shape[1]
        hbm = pl.BlockSpec(memory_space=pltpu.HBM)
        vmem = pl.BlockSpec(memory_space=pltpu.VMEM)
        flops = 2 * batch * tok * dim * (2 * dim + 2 * kv_dim) + 4 * batch * tok * n_cp * tok * n_heads * head
        return pl.pallas_call(
            functools.partial(block_kernel, n_cp, head),
            name='attention_block',
            out_shape=pltpu.VMEM(hidden.shape, hidden.dtype),
            in_specs=[hbm] * 7,
            out_specs=vmem,
            scratch_shapes=[
                pltpu.VMEM(positions.shape, jnp.int32),
                pltpu.VMEM(norm_gain.shape, BF16),
                pltpu.VMEM((head // 2, 2 * tok), F32),
                pltpu.VMEM((2, head // 2, 2 * tok), F32),
                pltpu.VMEM((2, head // 2, 2 * tok), F32),
                pltpu.VMEM((2, 2 * tok, dim), BF16),
                pltpu.VMEM(hidden.shape, BF16),
                pltpu.VMEM(w_query.shape, BF16),
                pltpu.VMEM(w_key.shape, BF16),
                pltpu.VMEM(w_value.shape, BF16),
                pltpu.VMEM((n_heads * head, dim), BF16),
                pltpu.VMEM((batch, n_heads // 2, kv_dim, 2 * tok), BF16),
                pltpu.VMEM((batch, n_cp, 2, tok, kv_dim), BF16),
                pltpu.VMEM((2, n_cp * tok, 4 * tok), F32),
                pltpu.VMEM((2 * tok, tok), F32),
                pltpu.VMEM((tok, n_heads * head), BF16),
                pltpu.SemaphoreType.DMA((batch,)),
                pltpu.SemaphoreType.DMA((6,)),
                pltpu.SemaphoreType.DMA((S_FWD + n_cp // 2 - 1, batch)),
                pltpu.SemaphoreType.DMA((batch, n_cp)),
            ],
            compiler_params=pltpu.CompilerParams(
                collective_id=0, has_side_effects=True, vmem_limit_bytes=40 * 1024 * 1024),
            cost_estimate=pl.CostEstimate(flops=flops, bytes_accessed=8_000_000, transcendentals=0),
        )(*[pltpu.with_memory_space_constraint(arg, pltpu.HBM) for arg in (
            hidden, positions, norm_gain, w_query, w_key, w_value, w_out.reshape(n_heads * head, dim))])

    act_spec = P('dp', 'cp', None)
    return jax.shard_map(local_block, mesh=mesh, in_specs=(act_spec, P('dp', 'cp'), P(), P(), P(), P(), P()), out_specs=act_spec, check_vma=False)
```

```python
import functools

import jax
import jax.numpy as jnp
import numpy as np
from jax import lax
from jax.experimental import pallas as pl
from jax.experimental.pallas import tpu as pltpu
from jax.sharding import PartitionSpec as P

F32 = jnp.float32
BF16 = jnp.bfloat16
MESH = pl.DeviceIdType.MESH
S_PART, S_RIGHT, S_LEFT, S_FAR, S_RELAY, S_FWD = 0, 1, 2, 3, 4, 5
AHEAD_2, AHEAD_3 = 3, 2
PACED = (3, 2, 3, 2)
FAR_0_TO_2 = (3, 6, 7)
FAR_1_TO_3 = (5, 6, 7)
HALF_FAR_1_TO_3 = (0, 3, 4)


def one_of(b, numbers):
    return functools.reduce(jnp.logical_or, [b == number for number in numbers], b < 0)


SPLIT = 2


def tdot(lhs, rhs, dims):
    return lax.dot_general(lhs, rhs, (dims, ((), ())), preferred_element_type=F32)


def rope(proj, cos, sin):
    half = cos.shape[0]
    first, second = proj[:half], proj[half:]
    return jnp.concatenate([first * cos - second * sin, second * cos + first * sin], axis=0).astype(BF16)


def block_kernel(n_cp, head, x_hbm, pos_hbm, gain_hbm, wq_hbm, wk_hbm, wv_hbm, wo_hbm, y_ref,
                 pos_ref, gain_ref, freq_s, cos_s, sin_s, normed_s, x_s, wq_s, wk_s, wv_s, wo_s, q_s, kv_s, score_s, bias_s, o_s,
                 x_sem, w_sem, send_sem, recv_sem):
    batch, tok, dim = x_hbm.shape
    kv_dim = wk_hbm.shape[1]
    n_kv = kv_dim // head
    n_heads = wq_hbm.shape[1] // head
    group = n_heads // n_kv
    n_pairs = n_heads // 2
    n_chips = n_cp // 2
    scale = float(head ** -0.5 * np.log2(np.e))

    me = lax.axis_index('cp')
    chip = me // 2
    core = me % 2
    partner = chip * 2 + 1 - core

    def x_copy(b):
        return pltpu.make_async_copy(x_hbm.at[b], x_s.at[b], x_sem.at[b])

    w_copies = [pltpu.make_async_copy(src, dst, w_sem.at[i]) for i, (src, dst) in enumerate(
        ((wk_hbm, wk_s), (wv_hbm, wv_s), (wq_hbm, wq_s), (wo_hbm, wo_s), (pos_hbm, pos_ref), (gain_hbm, gain_ref)))]
    w_copies[4].start()
    x_copy(0).start()
    x_copy(1).start()
    w_copies[5].start()
    w_copies[0].start()
    w_copies[1].start()
    w_copies[2].start()
    for b in range(2, batch):
        x_copy(b).start()
    w_copies[3].start()

    barrier = pltpu.get_barrier_semaphore()
    for d in range(1, n_cp):
        pl.semaphore_signal(barrier, inc=1, device_id={'cp': lax.rem(me + d, n_cp)}, device_id_type=MESH)

    key_i = lax.broadcasted_iota(jnp.int32, bias_s.shape, 0)
    tok_i = lax.broadcasted_iota(jnp.int32, bias_s.shape, 1)
    bias_s[...] = jnp.where(key_i <= tok_i + core * tok, 0.0, -jnp.inf).astype(F32)

    def send(b, src, dst, kind):
        return pltpu.make_async_remote_copy(
            src_ref=kv_s.at[b, src], dst_ref=kv_s.at[b, src],
            send_sem=send_sem.at[kind, b], recv_sem=recv_sem.at[b, src],
            device_id={'cp': dst}, device_id_type=MESH)

    def wait_recv(b, src):
        send(b, src, partner, S_PART).wait_recv()

    def on_chip(do):
        for j in range(n_chips):
            @pl.when(chip == j)
            def _():
                do(j)

    def direct_0_to_2(b):
        return one_of(b, FAR_0_TO_2)

    def direct_1_to_3(b):
        return one_of(b, FAR_1_TO_3) | ((core == 0) & one_of(b, HALF_FAR_1_TO_3))

    def own(j, b, do):
        if j == 0:
            do(send(b, me, 6 + core, S_LEFT))
            do(send(b, me, 2 + core, S_RIGHT))

            @pl.when(direct_0_to_2(b))
            def _():
                do(send(b, me, 4 + core, S_FAR))
        if j == 1:
            @pl.when(direct_1_to_3(b))
            def _():
                do(send(b, me, 6 + core, S_FAR))
            do(send(b, me, 4 + core, S_RIGHT))
        if j == 2:
            do(send(b, me, 6 + core, S_RIGHT))

    def stages(j, first, then):
        def forward(b, c):
            then(send(b, 2 * c + core, partner, S_FWD + c))

        def near(b):
            first(b, 2 * (j - 1) + core)
            forward(b, j - 1)

        def chip_2_right(b):
            first(b, 2 + core)

            @pl.when(jnp.logical_not(direct_1_to_3(b)))
            def _():
                then(send(b, 2 + core, 6 + core, S_RELAY))
            forward(b, 1)

        def chip_2_left(b):
            first(b, core)
            forward(b, 0)

        def chip_3_left(b):
            first(b, core)

            @pl.when(jnp.logical_not(direct_0_to_2(b)))
            def _():
                then(send(b, core, 4 + core, S_RELAY))
            forward(b, 0)

        def chip_3_right(b):
            near(b)
            first(b, 2 + core)
            forward(b, 1)

        return ((), ((1, near),), ((AHEAD_2, chip_2_right), (1, chip_2_left)), ((AHEAD_3, chip_3_left), (1, chip_3_right)))[j]

    w_copies[4].wait()
    w_copies[5].wait()
    row_i = lax.broadcasted_iota(jnp.int32, (head // 2, 2 * tok), 0)
    freq = jnp.ones((head // 2, 2 * tok), F32)
    for j in range(1, head // 2):
        freq = jnp.where(row_i == j, F32(10000.0 ** (-2.0 * j / head)), freq)
    freq_s[...] = freq
    w_copies[0].wait()
    w_copies[1].wait()

    def project_kv(p):
        for i in range(2):
            x_copy(2 * p + i).wait()
        x_pair = x_s[pl.ds(2 * p, 2)].reshape(2 * tok, dim).astype(F32)
        inv_rms = lax.rsqrt(jnp.mean(x_pair * x_pair, axis=-1, keepdims=True) + 1e-5)
        normed = (x_pair * inv_rms * gain_ref[...].astype(F32).reshape(1, dim)).astype(BF16)
        pos = jnp.concatenate([pos_ref[pl.ds(2 * p + i, 1), :] for i in range(2)], axis=1)
        angle = pos.astype(F32) * freq_s[...]
        cos, sin = jnp.cos(angle), jnp.sin(angle)
        k_t = tdot(wk_s[...], normed, ((0,), (1,)))
        v_t = tdot(wv_s[...], normed, ((0,), (1,))).astype(BF16)
        k_rot = jnp.concatenate([rope(k_t[g * head:(g + 1) * head], cos, sin) for g in range(n_kv)], axis=0)
        for i in range(2):
            kv_s[2 * p + i, me, 0] = k_rot[:, i * tok:(i + 1) * tok].T
            kv_s[2 * p + i, me, 1] = v_t[:, i * tok:(i + 1) * tok]
        normed_s[p % 2] = normed
        cos_s[p % 2] = cos
        sin_s[p % 2] = sin

    def start_own(p):
        def start(j):
            for i in range(2):
                @pl.when(2 * p + i < PACED[j])
                def _():
                    own(j, 2 * p + i, lambda copy: copy.start())
                send(2 * p + i, me, partner, S_PART).start()
        on_chip(start)

    def project_q(p):
        cos, sin = cos_s[p % 2], sin_s[p % 2]
        q_t = tdot(wq_s[...], normed_s[p % 2], ((0,), (1,)))
        zeros = jnp.zeros((head, tok), BF16)
        for n in range(n_heads):
            q_rot = rope(q_t[n * head:(n + 1) * head], cos, sin)
            col = (n % 2) * tok
            for i in range(2):
                for g in range(n_kv):
                    q_s[2 * p + i, n // 2, g * head:(g + 1) * head, col:col + tok] = (
                        q_rot[:, i * tok:(i + 1) * tok] if g == n // group else zeros)

    project_kv(0)
    pl.semaphore_wait(barrier, n_cp - 1)
    start_own(0)
    w_copies[2].wait()

    @pl.loop(1, batch // 2)
    def _(p):
        project_kv(p)
        project_q(p - 1)
        start_own(p)

    project_q(batch // 2 - 1)
    w_copies[3].wait()

    units = [(t, min(2, n_pairs - t)) for t in range(0, n_pairs, 2)]

    def scores(b, u, c, chunks):
        first_t, width = units[u]
        k_blk = jnp.concatenate([kv_s[b, 2 * c, 0], kv_s[b, 2 * c + 1, 0]], axis=0)
        q_unit = jnp.concatenate([q_s[b, first_t + i] for i in range(width)], axis=1)
        s_blk = tdot(k_blk, q_unit, ((1,), (0,)))
        if c == chunks - 1:
            s_blk = s_blk + jnp.concatenate([bias_s[...]] * (2 * width), axis=1)
        score_s[u % 2, 2 * tok * c:2 * tok * (c + 1), :2 * tok * width] = s_blk
        return jnp.max(s_blk, axis=0, keepdims=True)

    def attend(b, chunks, between):
        top = functools.reduce(jnp.maximum, [scores(b, 0, c, chunks) for c in range(chunks)])
        for u, (first_t, width) in enumerate(units):
            if u == SPLIT:
                between()
            probs, total, next_top = [], None, None
            for c in range(chunks):
                if u + 1 < len(units):
                    part = scores(b, u + 1, c, chunks)
                    next_top = part if c == 0 else jnp.maximum(next_top, part)
                prob = jnp.exp2((score_s[u % 2, 2 * tok * c:2 * tok * (c + 1), :2 * tok * width] - top) * scale)
                part = jnp.sum(prob, axis=0, keepdims=True)
                total = part if c == 0 else total + part
                probs.append(prob)
            inv = 1.0 / total
            for w in range(width):
                t = first_t + w
                lo, hi = (2 * t) // group, (2 * t + 1) // group
                v_rows = slice(lo * head, (hi + 1) * head)
                v_blk = jnp.concatenate([kv_s[b, s, 1][v_rows] for s in range(2 * chunks)], axis=1)
                pair = slice(2 * tok * w, 2 * tok * (w + 1))
                out = tdot(v_blk, jnp.concatenate([prob[:, pair] for prob in probs], axis=0), ((1,), (0,)))
                out_inv = inv[:, pair]
                halves = []
                for i in range(2):
                    row = ((2 * t + i) // group - lo) * head
                    cols = slice(i * tok, (i + 1) * tok)
                    halves.append(out[row:row + head, cols] * out_inv[:, cols])
                o_s[:, 2 * t * head:2 * (t + 1) * head] = jnp.concatenate(halves, axis=0).T.astype(BF16)
            top = next_top

    def pass_on(j):
        return stages(j, wait_recv, lambda copy: copy.start())

    def prologue(j):
        for ahead, stage in pass_on(j):
            for b in range(ahead):
                stage(jnp.int32(b))

    on_chip(prologue)

    @pl.loop(0, batch)
    def _(b):
        def one_chip(j):
            @pl.when(b + PACED[j] < batch)
            def _():
                own(j, b + PACED[j], lambda copy: copy.start())
            wait_recv(b, partner)
            for c in range(j):
                wait_recv(b, 2 * c + 1 - core)

            def between():
                for ahead, stage in pass_on(j):
                    @pl.when(b + ahead < batch)
                    def _():
                        stage(b + ahead)
            attend(b, j + 1, between)

        on_chip(one_chip)
        proj = tdot(o_s[...], wo_s[...], ((1,), (0,)))
        y_ref[b] = (x_s[b].astype(F32) + proj).astype(BF16)

    @pl.loop(0, batch)
    def _(b):
        def one_chip(j):
            send(b, me, partner, S_PART).wait_send()
            own(j, b, lambda copy: copy.wait_send())
            for _, stage in stages(j, lambda b, src: None, lambda copy: copy.wait_send()):
                stage(b)
        on_chip(one_chip)


def solution(mesh):
    n_cp = mesh.shape['cp']

    def local_block(hidden, positions, norm_gain, w_query, w_key, w_value, w_out):
        batch, tok, dim = hidden.shape
        n_heads, head, _ = w_out.shape
        kv_dim = w_key.shape[1]
        hbm = pl.BlockSpec(memory_space=pltpu.HBM)
        vmem = pl.BlockSpec(memory_space=pltpu.VMEM)
        flops = 2 * batch * tok * dim * (2 * dim + 2 * kv_dim) + 4 * batch * tok * n_cp * tok * n_heads * head
        return pl.pallas_call(
            functools.partial(block_kernel, n_cp, head),
            name='attention_block',
            out_shape=pltpu.VMEM(hidden.shape, hidden.dtype),
            in_specs=[hbm] * 7,
            out_specs=vmem,
            scratch_shapes=[
                pltpu.VMEM(positions.shape, jnp.int32),
                pltpu.VMEM(norm_gain.shape, BF16),
                pltpu.VMEM((head // 2, 2 * tok), F32),
                pltpu.VMEM((2, head // 2, 2 * tok), F32),
                pltpu.VMEM((2, head // 2, 2 * tok), F32),
                pltpu.VMEM((2, 2 * tok, dim), BF16),
                pltpu.VMEM(hidden.shape, BF16),
                pltpu.VMEM(w_query.shape, BF16),
                pltpu.VMEM(w_key.shape, BF16),
                pltpu.VMEM(w_value.shape, BF16),
                pltpu.VMEM((n_heads * head, dim), BF16),
                pltpu.VMEM((batch, n_heads // 2, kv_dim, 2 * tok), BF16),
                pltpu.VMEM((batch, n_cp, 2, tok, kv_dim), BF16),
                pltpu.VMEM((2, n_cp * tok, 4 * tok), F32),
                pltpu.VMEM((2 * tok, tok), F32),
                pltpu.VMEM((tok, n_heads * head), BF16),
                pltpu.SemaphoreType.DMA((batch,)),
                pltpu.SemaphoreType.DMA((6,)),
                pltpu.SemaphoreType.DMA((S_FWD + n_cp // 2 - 1, batch)),
                pltpu.SemaphoreType.DMA((batch, n_cp)),
            ],
            compiler_params=pltpu.CompilerParams(
                collective_id=0, has_side_effects=True, vmem_limit_bytes=40 * 1024 * 1024),
            cost_estimate=pl.CostEstimate(flops=flops, bytes_accessed=8_000_000, transcendentals=0),
        )(*[pltpu.with_memory_space_constraint(arg, pltpu.HBM) for arg in (
            hidden, positions, norm_gain, w_query, w_key, w_value, w_out.reshape(n_heads * head, dim))])

    act_spec = P('dp', 'cp', None)
    return jax.shard_map(local_block, mesh=mesh, in_specs=(act_spec, P('dp', 'cp'), P(), P(), P(), P(), P()), out_specs=act_spec, check_vma=False)
```
